8 devices in a mesh: dp: 2 (over z, y), tp: 4 (over x, core).
Axes of the slice: x: 2, y: 2, z: 1, core: 2. Of those that a mesh axis runs over, the one named last changes fastest.
Arguments:
- tokens: int32 [2, 256], P('dp'), parts along dimension 0
- positions: int32 [2, 256], P('dp'), parts along dimension 0
- embed_table: bfloat16 [128256, 3072], P('tp')
- w_query: bfloat16 [3072, 24, 128], P(None, 'tp')
- w_key: bfloat16 [3072, 8, 128], P(None, 'tp')
- w_value: bfloat16 [3072, 8, 128], P(None, 'tp')
- w_out: bfloat16 [24, 128, 3072], P('tp')
- w_gate: bfloat16 [3072, 8192], P(None, 'tp')
- w_up: bfloat16 [3072, 8192], P(None, 'tp')
- w_down: bfloat16 [8192, 3072], P('tp')
- norm_pre_att: float32 [3072], replicated
- norm_post_att: float32 [3072], replicated
- norm_pre_ffw: float32 [3072], replicated
- norm_post_ffw: float32 [3072], replicated
Outputs:
- output: bfloat16 [2, 256, 3072], P('dp', 'tp'), parts along dimension 0
There are 2 independent parts. The reference program is written for one: setup_inputs(seed, part) draws one part's arguments, and reference() takes and returns one part's arrays. A program takes and returns all parts, laid end to end along the dimension named above; an argument that names none is the same for every part.
All inputs are finite; a program needn't handle non-finite values.
Results may differ from the reference program's by a relative error of at most 0.02.
Values are sent between devices in bfloat16 or wider.
A program may use at most 1 GiB of HBM per device.

```python
import jax
import jax.numpy as jnp
from jax import lax

BATCH_SIZE = 1
SEQ_LEN = 256
MODEL_DIM = 3072
N_HEADS = 24
KV_HEADS = 8
HEAD_DIM = 128
FFN_DIM = 8192
VOCAB_SIZE = 128256
WINDOW = 4096
QUERY_SCALAR = 256

GROUP_SIZE = N_HEADS // KV_HEADS
QUERY_BLOCK = min(128, SEQ_LEN)
KEY_SPAN = min(SEQ_LEN, WINDOW + QUERY_BLOCK)
SOFT_CAP = 50.0
NORM_EPS = 1e-6
ROPE_BASE = 10000.0


def setup_inputs(seed: int = 0, part: int = 0) -> dict:
    root_key = jax.random.key(seed)
    key_list = jax.random.split(root_key, 11)
    part_keys = jax.random.split(jax.random.fold_in(root_key, part), 5)
    grid_shape = (BATCH_SIZE, SEQ_LEN)
    choice = jax.random.randint(part_keys[0], grid_shape, 0, 4, dtype=jnp.int32)
    hot_ids = jax.random.randint(part_keys[1], grid_shape, 0, VOCAB_SIZE // 4, dtype=jnp.int32)
    any_ids = jax.random.randint(part_keys[2], grid_shape, 0, VOCAB_SIZE, dtype=jnp.int32)
    tokens = jnp.where(choice < 3, hot_ids, any_ids)
    tokens = tokens.at[0, 0].set(VOCAB_SIZE - 1).at[0, 1].set(0)
    pos_step = max(1, (2 * WINDOW) // SEQ_LEN)
    pos_gaps = jax.random.randint(part_keys[3], grid_shape, 1, 2 * pos_step + 1, dtype=jnp.int32)
    first_pos = jax.random.randint(part_keys[4], (BATCH_SIZE, 1), 0, WINDOW, dtype=jnp.int32)
    positions = (first_pos + jnp.cumsum(pos_gaps, axis=1) - pos_gaps[:, :1]).astype(jnp.int32)

    def draw_weight(key_index, w_shape, fan_in):
        raw_noise = jax.random.normal(key_list[key_index], w_shape, jnp.float32)
        return (raw_noise * fan_in ** -0.5).astype(jnp.bfloat16)

    def table_rows(row_group):
        raw_noise = jax.random.normal(jax.random.fold_in(key_list[0], row_group), (VOCAB_SIZE // 8, MODEL_DIM), jnp.float32)
        return (raw_noise * MODEL_DIM ** -0.5).astype(jnp.bfloat16)

    embed_table = lax.map(table_rows, jnp.arange(8)).reshape(VOCAB_SIZE, MODEL_DIM)
    norm_draws = 0.3 * jax.random.normal(key_list[8], (4, MODEL_DIM), jnp.float32)
    return {
        "tokens": tokens,
        "positions": positions,
        "embed_table": embed_table,
        "w_query": draw_weight(1, (MODEL_DIM, N_HEADS, HEAD_DIM), MODEL_DIM),
        "w_key": draw_weight(2, (MODEL_DIM, KV_HEADS, HEAD_DIM), MODEL_DIM),
        "w_value": draw_weight(3, (MODEL_DIM, KV_HEADS, HEAD_DIM), MODEL_DIM),
        "w_out": draw_weight(4, (N_HEADS, HEAD_DIM, MODEL_DIM), N_HEADS * HEAD_DIM),
        "w_gate": draw_weight(5, (MODEL_DIM, FFN_DIM), MODEL_DIM),
        "w_up": draw_weight(6, (MODEL_DIM, FFN_DIM), MODEL_DIM),
        "w_down": draw_weight(7, (FFN_DIM, MODEL_DIM), FFN_DIM),
        "norm_pre_att": norm_draws[0],
        "norm_post_att": norm_draws[1],
        "norm_pre_ffw": norm_draws[2],
        "norm_post_ffw": norm_draws[3],
    }


def rms_norm(hidden, norm_scale):
    hidden = hidden.astype(jnp.float32)
    mean_sq = jnp.mean(hidden * hidden, axis=-1, keepdims=True)
    return (hidden * lax.rsqrt(mean_sq + NORM_EPS) * (1.0 + norm_scale)).astype(jnp.bfloat16)


def apply_rope(states, positions):
    half_dim = HEAD_DIM // 2
    inv_freq = ROPE_BASE ** (-2.0 * jnp.arange(half_dim, dtype=jnp.float32) / HEAD_DIM)
    angles = positions.astype(jnp.float32)[:, :, None] * inv_freq
    cos_tab = jnp.cos(angles)[:, :, None, :]
    sin_tab = jnp.sin(angles)[:, :, None, :]
    lower_half = states[..., :half_dim]
    upper_half = states[..., half_dim:]
    return jnp.concatenate([lower_half * cos_tab - upper_half * sin_tab, upper_half * cos_tab + lower_half * sin_tab], axis=-1)


def project(act_rows, weight, out_shape):
    flat_rows = act_rows.reshape(-1, act_rows.shape[-1])
    flat_w = weight.reshape(act_rows.shape[-1], -1)
    return jnp.dot(flat_rows, flat_w, preferred_element_type=jnp.float32).reshape(out_shape)


def attend(q_states, k_states, v_states, positions):
    n_blocks = SEQ_LEN // QUERY_BLOCK

    def one_block(block_idx):
        q_start = block_idx * QUERY_BLOCK
        k_start = jnp.maximum(q_start + QUERY_BLOCK - KEY_SPAN, 0)
        q_blk = lax.dynamic_slice_in_dim(q_states, q_start, QUERY_BLOCK, axis=1)
        k_blk = lax.dynamic_slice_in_dim(k_states, k_start, KEY_SPAN, axis=1)
        v_blk = lax.dynamic_slice_in_dim(v_states, k_start, KEY_SPAN, axis=1)
        q_pos = lax.dynamic_slice_in_dim(positions, q_start, QUERY_BLOCK, axis=1)
        k_pos = lax.dynamic_slice_in_dim(positions, k_start, KEY_SPAN, axis=1)
        scores = jnp.einsum("bqkgd,blkd->bkgql", q_blk.astype(jnp.float32), k_blk.astype(jnp.float32))
        capped = SOFT_CAP * jnp.tanh(scores / SOFT_CAP)
        offset = q_pos[:, :, None] - k_pos[:, None, :]
        keep_mask = (offset >= 0) & (offset < WINDOW)
        capped = jnp.where(keep_mask[:, None, None, :, :], capped, -1e30)
        att_probs = jax.nn.softmax(capped, axis=-1).astype(jnp.bfloat16)
        att_mix = jnp.einsum("bkgql,blkd->bqkgd", att_probs.astype(jnp.float32), v_blk.astype(jnp.float32))
        return att_mix.astype(jnp.bfloat16)

    blocks = lax.map(one_block, jnp.arange(n_blocks))
    return jnp.moveaxis(blocks, 0, 1).reshape(BATCH_SIZE, SEQ_LEN, KV_HEADS, GROUP_SIZE, HEAD_DIM)


def reference(tokens, positions, embed_table, w_query, w_key, w_value, w_out, w_gate, w_up, w_down, norm_pre_att, norm_post_att, norm_pre_ffw, norm_post_ffw):
    normalizer = jnp.sqrt(jnp.float32(MODEL_DIM)).astype(jnp.bfloat16).astype(jnp.float32)
    looked = jnp.take(embed_table, tokens, axis=0)
    embeds = (looked.astype(jnp.float32) * normalizer).astype(jnp.bfloat16)
    attn_in = rms_norm(embeds, norm_pre_att)
    heads_shape = (BATCH_SIZE, SEQ_LEN, N_HEADS, HEAD_DIM)
    kv_shape = (BATCH_SIZE, SEQ_LEN, KV_HEADS, HEAD_DIM)
    q_states = apply_rope(project(attn_in, w_query, heads_shape), positions) * QUERY_SCALAR ** -0.5
    q_states = q_states.astype(jnp.bfloat16).reshape(BATCH_SIZE, SEQ_LEN, KV_HEADS, GROUP_SIZE, HEAD_DIM)
    k_states = apply_rope(project(attn_in, w_key, kv_shape), positions).astype(jnp.bfloat16)
    v_states = project(attn_in, w_value, kv_shape).astype(jnp.bfloat16)
    att_mix = attend(q_states, k_states, v_states, positions)
    model_shape = (BATCH_SIZE, SEQ_LEN, MODEL_DIM)
    att_flat = att_mix.reshape(BATCH_SIZE, SEQ_LEN, N_HEADS * HEAD_DIM)
    att_proj = project(att_flat, w_out, model_shape).astype(jnp.bfloat16)
    resid_one = (embeds.astype(jnp.float32) + rms_norm(att_proj, norm_post_att).astype(jnp.float32)).astype(jnp.bfloat16)
    mlp_in = rms_norm(resid_one, norm_pre_ffw)
    ffn_shape = (BATCH_SIZE, SEQ_LEN, FFN_DIM)
    gate_pre = project(mlp_in, w_gate, ffn_shape)
    up_proj = project(mlp_in, w_up, ffn_shape)
    ffn_act = (jax.nn.gelu(gate_pre, approximate=True) * up_proj).astype(jnp.bfloat16)
    down_proj = project(ffn_act, w_down, model_shape).astype(jnp.bfloat16)
    return (resid_one.astype(jnp.float32) + rms_norm(down_proj, norm_post_ffw).astype(jnp.float32)).astype(jnp.bfloat16)
```

```python
import functools

import jax
import jax.numpy as jnp
import numpy as np
from jax import lax
from jax.experimental import pallas as pl
from jax.experimental.pallas import tpu as pltpu
from jax.sharding import PartitionSpec as P

WINDOW = 4096
QUERY_SCALE = 256.0 ** -0.5
SOFT_CAP = 50.0
NORM_EPS = 1e-6
ROPE_BASE = 10000.0
SEQ = 256
DIM = 3072
FFN = 2048
CHUNK = 128
HALF = 64
ROWP = 16
NRP = HALF // ROWP
COLP = 1024
NCP = DIM // COLP
BF = jnp.bfloat16
F32 = jnp.float32


def rms_rows(u, gain):
    mean_sq = jnp.mean(u * u, axis=-1, keepdims=True)
    return (u * lax.rsqrt(mean_sq + NORM_EPS) * gain).astype(BF)


def layer_kernel(looked, scale_col, cos_tab, sin_tab, pos_col, pos_row, wq_hbm, wk_hbm, wv_hbm, wo_hbm, wg_hbm, wu_hbm, wd_hbm, g1, g2, g3, g4,
                 out,
                 wqkv, wo, wg, wu, wd, part, ssum, rd, rxe, rxy, rxz, act, resid, hid, qs, ks, vs, os_, f32buf,
                 wsem, esend, erecv, exsend, exrecv, asend, arecv, ysend, yrecv, yxsend, yxrecv, msend, mrecv, zsend, zrecv, zxsend, zxrecv):
    tp = lax.axis_index("tp")
    chip = tp // 2
    core = tp % 2
    partner = chip * 2 + (1 - core)
    peer = (1 - chip) * 2 + core

    def remote(src, dst, ssem, rsem, dev):
        return pltpu.make_async_remote_copy(src_ref=src, dst_ref=dst, send_sem=ssem, recv_sem=rsem, device_id={"tp": dev}, device_id_type=pl.DeviceIdType.MESH)

    look_cp = pltpu.make_async_copy(looked, part, wsem.at[0])
    look_cp.start()
    raw_cps = []
    for i in range(3):
        raw_cps.append(pltpu.make_async_copy(wk_hbm.at[pl.ds(2048 * i, 2048)], wd.at[:, pl.ds(128 * i, 128)], wsem.at[1 + i]))
        raw_cps.append(pltpu.make_async_copy(wv_hbm.at[pl.ds(2048 * i, 2048)], wd.at[:, pl.ds(384 + 128 * i, 128)], wsem.at[4 + i]))
    for cp in raw_cps:
        cp.start()
    q_cps = [pltpu.make_async_copy(wq_hbm.at[h], wqkv.at[:, pl.ds(128 * h, 128)], wsem.at[7 + h]) for h in range(6)]
    for cp in q_cps:
        cp.start()
    wo_cp = pltpu.make_async_copy(wo_hbm, wo, wsem.at[13])
    wo_cp.start()
    wg_cp = pltpu.make_async_copy(wg_hbm, wg, wsem.at[14])
    wu_cp = pltpu.make_async_copy(wu_hbm, wu, wsem.at[15])
    wd_cp = pltpu.make_async_copy(wd_hbm, wd, wsem.at[16])
    wg_cp.start()
    wu_cp.start()

    barrier = pltpu.get_barrier_semaphore()
    for dev in (partner, peer):
        pl.semaphore_signal(barrier, inc=1, device_id={"tp": dev}, device_id_type=pl.DeviceIdType.MESH)
    pl.semaphore_wait(barrier, 2)

    def own(k):
        return pl.multiple_of(CHUNK * k + HALF * core, HALF)

    def theirs(k):
        return pl.multiple_of(CHUNK * k + HALF * (1 - core), HALF)

    look_cp.wait()

    def e_d2d(k, j):
        return remote(part.at[pl.ds(theirs(k) + ROWP * j, ROWP)], rd.at[k, pl.ds(ROWP * j, ROWP)], esend.at[k, j], erecv.at[k, j], partner)

    def e_x(k, j):
        sl = pl.ds(ROWP * j, ROWP)
        return remote(ssum.at[k, sl], rxe.at[k, sl], exsend.at[k, j], exrecv.at[k, j], peer)

    def a_d2d(k, j):
        sl = pl.ds(own(k) + ROWP * j, ROWP)
        return remote(act.at[sl], act.at[sl], asend.at[k, j], arecv.at[k, j], partner)

    def a_in(k, j):
        sl = pl.ds(theirs(k) + ROWP * j, ROWP)
        return remote(act.at[sl], act.at[sl], asend.at[k, j], arecv.at[k, j], partner)

    def scale_rows(row):
        sl = pl.ds(row, ROWP)
        part[sl, :] = (part[sl, :].astype(F32) * scale_col[sl, :]).astype(BF)

    for k in range(2):
        for j in range(NRP):
            scale_rows(pl.multiple_of(theirs(k) + ROWP * j, ROWP))
            e_d2d(k, j).start()
        for j in range(NRP):
            scale_rows(pl.multiple_of(own(k) + ROWP * j, ROWP))
    for k in range(2):
        for j in range(NRP):
            sl = pl.ds(ROWP * j, ROWP)
            e_d2d(k, j).wait_recv()
            ssum[k, sl, :] = part[pl.ds(pl.multiple_of(own(k) + ROWP * j, ROWP), ROWP), :] + rd[k, sl, :]
            e_x(k, j).start()

    for cp in raw_cps:
        cp.wait()
    for w in range(2):
        for i in range(3):
            def split_heads(b, carry, w=w, i=i):
                row = pl.multiple_of(b * 512, 512)
                f32buf[...] = wd[pl.ds(row, 512), pl.ds(384 * w + 128 * i, 128)].astype(F32)
                dst = pl.ds(pl.multiple_of(1024 * i + b * 256, 256), 256)
                for h in range(2):
                    wqkv[dst, pl.ds(768 + 256 * w + 128 * h, 128)] = f32buf[pl.ds(h, 256, stride=2), :].astype(BF)
                return carry
            lax.fori_loop(0, 4, split_heads, 0)
    wd_cp.start()

    gain1 = 1.0 + g1[...]
    gain2 = 1.0 + g2[...]
    gain3 = 1.0 + g3[...]
    gain4 = 1.0 + g4[...]

    def embed_chunk(k):
        for j in range(NRP):
            sl = pl.ds(ROWP * j, ROWP)
            e_x(k, j).wait_recv()
            emb = ssum[k, sl, :] + rxe[k, sl, :]
            resid[k, sl, :] = emb
            act[pl.ds(pl.multiple_of(own(k) + ROWP * j, ROWP), ROWP), :] = rms_rows(emb.astype(F32), gain1)
            a_d2d(k, j).start()
        for j in range(NRP):
            a_in(k, j).wait_recv()

    def qkv_chunk(k):
        rows = pl.ds(CHUNK * k, CHUNK)
        cos_c = cos_tab[rows, :]
        sin_c = sin_tab[rows, :]

        def rope(u):
            return u * cos_c + pltpu.roll(u, 64, 1) * sin_c

        for b in range(5):
            prod = jnp.dot(act[rows, :], wqkv[:, pl.ds(256 * b, 256)], preferred_element_type=F32)
            for h in range(2):
                u = prod[:, 128 * h:128 * h + 128]
                if b < 3:
                    qs[2 * b + h] = (rope(u) * QUERY_SCALE).astype(BF)
                elif b == 3:
                    ks[h, rows, :] = rope(u).astype(BF)
                else:
                    vs[h, rows, :] = u.astype(BF)

    def attend_chunk(k):
        span = CHUNK * (k + 1)
        offset = pos_col[pl.ds(CHUNK * k, CHUNK), :] - pos_row[:, pl.ds(0, span)]
        keep = (offset >= 0) & (offset < WINDOW)
        for g in range(2):
            kk = ks[g, pl.ds(0, span), :]
            vv = vs[g, pl.ds(0, span), :]
            for i in range(3):
                s = lax.dot_general(qs[3 * g + i], kk, (((1,), (1,)), ((), ())), preferred_element_type=F32)
                c = SOFT_CAP * jnp.tanh(s * (1.0 / SOFT_CAP))
                e = jnp.where(keep, jnp.exp(c), 0.0)
                pr = (e * (1.0 / jnp.sum(e, axis=-1, keepdims=True))).astype(BF)
                o = jnp.dot(pr, vv, preferred_element_type=F32)
                os_[:, pl.ds(128 * (3 * g + i), 128)] = o.astype(BF)

    def y_d2d(k, n):
        cs = pl.ds(COLP * n, COLP)
        return remote(part.at[pl.ds(theirs(k), HALF), cs], rd.at[k, :, cs], ysend.at[k, n], yrecv.at[k, n], partner)

    def y_x(k, n):
        cs = pl.ds(COLP * n, COLP)
        return remote(ssum.at[k, :, cs], rxy.at[k, :, cs], yxsend.at[k, n], yxrecv.at[k, n], peer)

    def out_chunk(k):
        rows = pl.ds(CHUNK * k, CHUNK)
        for j in range(NRP):
            e_d2d(k, j).wait_send()
        for n in range(NCP):
            def col(b, carry, n=n):
                cs = pl.ds(pl.multiple_of(COLP * n + 256 * b, 256), 256)
                part[rows, cs] = jnp.dot(os_[...], wo[:, cs], preferred_element_type=F32).astype(BF)
                return carry
            lax.fori_loop(0, COLP // 256, col, 0)
            y_d2d(k, n).start()
        for j in range(NRP):
            e_x(k, j).wait_send()
        for n in range(NCP):
            cs = pl.ds(COLP * n, COLP)
            y_d2d(k, n).wait_recv()
            ssum[k, :, cs] = (part[pl.ds(own(k), HALF), cs].astype(F32) + rd[k, :, cs].astype(F32)).astype(BF)
            y_x(k, n).start()

    def mid_chunk(k):
        for j in range(NRP):
            a_d2d(k, j).wait_send()
        for n in range(NCP):
            y_x(k, n).wait_recv()
        for j in range(NRP):
            sl = pl.ds(ROWP * j, ROWP)
            y = (ssum[k, sl, :].astype(F32) + rxy[k, sl, :].astype(F32)).astype(BF).astype(F32)
            x1 = (resid[k, sl, :].astype(F32) + rms_rows(y, gain2).astype(F32)).astype(BF)
            resid[k, sl, :] = x1
            act[pl.ds(pl.multiple_of(own(k) + ROWP * j, ROWP), ROWP), :] = rms_rows(x1.astype(F32), gain3)
            m_d2d(k, j).start()
        for j in range(NRP):
            m_in(k, j).wait_recv()

    def m_d2d(k, j):
        sl = pl.ds(own(k) + ROWP * j, ROWP)
        return remote(act.at[sl], act.at[sl], msend.at[k, j], mrecv.at[k, j], partner)

    def m_in(k, j):
        sl = pl.ds(theirs(k) + ROWP * j, ROWP)
        return remote(act.at[sl], act.at[sl], msend.at[k, j], mrecv.at[k, j], partner)

    def z_d2d(k, n):
        cs = pl.ds(COLP * n, COLP)
        return remote(part.at[pl.ds(theirs(k), HALF), cs], rd.at[k, :, cs], zsend.at[k, n], zrecv.at[k, n], partner)

    def z_x(k, n):
        cs = pl.ds(COLP * n, COLP)
        return remote(ssum.at[k, :, cs], rxz.at[:, cs], zxsend.at[n], zxrecv.at[n], peer)

    def ffn_chunk(k):
        rows = pl.ds(CHUNK * k, CHUNK)

        def up(b, carry):
            cs = pl.ds(pl.multiple_of(256 * b, 256), 256)
            gate = jnp.dot(act[rows, :], wg[:, cs], preferred_element_type=F32)
            upp = jnp.dot(act[rows, :], wu[:, cs], preferred_element_type=F32)
            hid[:, cs] = (jax.nn.gelu(gate, approximate=True) * upp).astype(BF)
            return carry
        lax.fori_loop(0, FFN // 256, up, 0)
        for n in range(NCP):
            y_d2d(k, n).wait_send()
        if k == 0:
            wd_cp.wait()
        for n in range(NCP):
            def col(b, carry, n=n):
                cs = pl.ds(pl.multiple_of(COLP * n + 256 * b, 256), 256)
                part[rows, cs] = jnp.dot(hid[...], wd[:, cs], preferred_element_type=F32).astype(BF)
                return carry
            lax.fori_loop(0, COLP // 256, col, 0)
            z_d2d(k, n).start()
        for n in range(NCP):
            y_x(k, n).wait_send()
        for n in range(NCP):
            cs = pl.ds(COLP * n, COLP)
            z_d2d(k, n).wait_recv()
            ssum[k, :, cs] = (part[pl.ds(own(k), HALF), cs].astype(F32) + rd[k, :, cs].astype(F32)).astype(BF)

            @pl.when(chip != k)
            def _(k=k, n=n):
                z_x(k, n).start()

    embed_chunk(0)
    for cp in q_cps:
        cp.wait()
    qkv_chunk(0)
    attend_chunk(0)
    wo_cp.wait()
    out_chunk(0)
    embed_chunk(1)
    qkv_chunk(1)
    attend_chunk(1)
    out_chunk(1)
    mid_chunk(0)
    wg_cp.wait()
    wu_cp.wait()
    ffn_chunk(0)
    mid_chunk(1)
    ffn_chunk(1)
    for n in range(NCP):
        z_x(0, n).wait_recv()
    for j in range(NRP):
        sl = pl.ds(ROWP * j, ROWP)
        z = (ssum[chip, sl, :].astype(F32) + rxz[sl, :].astype(F32)).astype(BF).astype(F32)
        out[0, sl, :] = (resid[chip, sl, :].astype(F32) + rms_rows(z, gain4).astype(F32)).astype(BF)
    for k in range(2):
        for j in range(NRP):
            m_d2d(k, j).wait_send()
        for n in range(NCP):
            z_d2d(k, n).wait_send()
    for n in range(NCP):
        z_x(0, n).wait_send()


def solution(mesh):
    in_specs = (P("dp", None), P("dp", None), P("tp", None), P(None, "tp", None), P(None, "tp", None), P(None, "tp", None), P("tp", None, None), P(None, "tp"), P(None, "tp"), P("tp", None), P(None), P(None), P(None), P(None))

    vm = pl.BlockSpec(memory_space=pltpu.VMEM)
    hb = pl.BlockSpec(memory_space=pl.ANY)
    dma = pltpu.SemaphoreType.DMA
    kernel = pl.pallas_call(
        layer_kernel,
        out_shape=jax.ShapeDtypeStruct((1, HALF, DIM), BF),
        in_specs=[hb, vm, vm, vm, vm, vm] + [hb] * 7 + [vm] * 4,
        out_specs=vm,
        scratch_shapes=[
            pltpu.VMEM((DIM, 1280), BF),
            pltpu.VMEM((768, DIM), BF),
            pltpu.VMEM((DIM, FFN), BF),
            pltpu.VMEM((DIM, FFN), BF),
            pltpu.VMEM((FFN, DIM), BF),
            pltpu.VMEM((SEQ, DIM), BF),
            pltpu.VMEM((2, HALF, DIM), BF),
            pltpu.VMEM((2, HALF, DIM), BF),
            pltpu.VMEM((2, HALF, DIM), BF),
            pltpu.VMEM((2, HALF, DIM), BF),
            pltpu.VMEM((HALF, DIM), BF),
            pltpu.VMEM((SEQ, DIM), BF),
            pltpu.VMEM((2, HALF, DIM), BF),
            pltpu.VMEM((CHUNK, FFN), BF),
            pltpu.VMEM((6, CHUNK, 128), BF),
            pltpu.VMEM((2, SEQ, 128), BF),
            pltpu.VMEM((2, SEQ, 128), BF),
            pltpu.VMEM((CHUNK, 768), BF),
            pltpu.VMEM((512, 128), F32),
            dma((17,)),
            dma((2, NRP)), dma((2, NRP)),
            dma((2, NRP)), dma((2, NRP)),
            dma((2, NRP)), dma((2, NRP)),
            dma((2, NCP)), dma((2, NCP)),
            dma((2, NCP)), dma((2, NCP)),
            dma((2, NRP)), dma((2, NRP)),
            dma((2, NCP)), dma((2, NCP)),
            dma((NCP,)), dma((NCP,)),
        ],
        compiler_params=pltpu.CompilerParams(collective_id=0, has_side_effects=True, vmem_limit_bytes=67043328),
        name="decoder_layer",
    )

    def device_step(tokens, positions, embed_block, w_query, w_key, w_value, w_out, w_gate, w_up, w_down, g1, g2, g3, g4):
        dev_rank = lax.axis_index("tp")
        vocab_local, model_dim = embed_block.shape
        ids = tokens[0] - dev_rank * vocab_local
        in_block = (ids >= 0) & (ids < vocab_local)
        looked = jnp.take(embed_block, jnp.clip(ids, 0, vocab_local - 1), axis=0, mode="clip")
        normalizer = float(np.asarray(np.sqrt(np.float32(model_dim)), dtype=jnp.bfloat16))
        scale_col = jnp.where(in_block, jnp.float32(normalizer), jnp.float32(0.0))[:, None]
        inv_freq = ROPE_BASE ** (-2.0 * jnp.arange(64, dtype=F32) / 128)
        angles = positions[0].astype(F32)[:, None] * inv_freq
        cos_h, sin_h = jnp.cos(angles), jnp.sin(angles)
        cos_tab = jnp.concatenate([cos_h, cos_h], axis=1)
        sin_tab = jnp.concatenate([-sin_h, sin_h], axis=1)
        return kernel(looked, scale_col, cos_tab, sin_tab, positions.reshape(SEQ, 1), positions,
                      w_query.transpose(1, 0, 2), w_key.reshape(2 * model_dim, 128), w_value.reshape(2 * model_dim, 128), w_out.reshape(768, model_dim),
                      w_gate, w_up, w_down, g1[None], g2[None], g3[None], g4[None])

    return jax.shard_map(device_step, mesh=mesh, in_specs=in_specs, out_specs=P("dp", "tp", None), check_vma=False)
```

```python
import functools

import jax
import jax.numpy as jnp
import numpy as np
from jax import lax
from jax.experimental import pallas as pl
from jax.experimental.pallas import tpu as pltpu
from jax.sharding import PartitionSpec as P

WINDOW = 4096
QUERY_SCALE = 256.0 ** -0.5
SOFT_CAP = 50.0
NORM_EPS = 1e-6
ROPE_BASE = 10000.0
SEQ = 256
DIM = 3072
FFN = 2048
CHUNK = 128
HALF = 64
QTR = 32
UPB = 512
VOCAB_LOCAL = 32064
NORMALIZER = float(np.asarray(np.sqrt(np.float32(DIM)), dtype=jnp.bfloat16))
ROWP = 16
NRP = HALF // ROWP
COLP = 1024
NCP = DIM // COLP
BF = jnp.bfloat16
F32 = jnp.float32


def rms_rows(u, gain):
    mean_sq = jnp.mean(u * u, axis=-1, keepdims=True)
    return (u * lax.rsqrt(mean_sq + NORM_EPS) * gain).astype(BF)


def column_of(row_f32):
    diag = lax.broadcasted_iota(jnp.int32, (128, 128), 0) == lax.broadcasted_iota(jnp.int32, (128, 128), 1)
    return jnp.sum(jnp.where(diag, jnp.broadcast_to(row_f32, (128, 128)), 0.0), axis=1, keepdims=True)


def layer_kernel(looked, tok_row, pos_row, cos_tab, sin_tab, wq_hbm, wk_hbm, wv_hbm, wo_hbm, wg_hbm, wu_hbm, wd_hbm, g1, g2, g3, g4,
                 out,
                 wqkv, wo, wg, wu, wd, part, ssum, rd, rxe, rxy, rxz, act, resid, hid, qs, ks, vs, os_, f32buf, scale_col, pos_col,
                 wsem, esend, erecv, exsend, exrecv, asend, arecv, ysend, yrecv, yxsend, yxrecv, msend, mrecv, zsend, zrecv, zxsend, zxrecv):
    tp = lax.axis_index("tp")
    chip = tp // 2
    core = tp % 2
    partner = chip * 2 + (1 - core)
    peer = (1 - chip) * 2 + core

    def remote(src, dst, ssem, rsem, dev):
        return pltpu.make_async_remote_copy(src_ref=src, dst_ref=dst, send_sem=ssem, recv_sem=rsem, device_id={"tp": dev}, device_id_type=pl.DeviceIdType.MESH)

    barrier = pltpu.get_barrier_semaphore()
    for dev in (partner, peer):
        pl.semaphore_signal(barrier, inc=1, device_id={"tp": dev}, device_id_type=pl.DeviceIdType.MESH)

    look_cp = pltpu.make_async_copy(looked, part, wsem.at[0])
    look_cp.start()
    raw_cps = []
    for i in range(3):
        raw_cps.append(pltpu.make_async_copy(wk_hbm.at[pl.ds(2048 * i, 2048)], wd.at[:, pl.ds(128 * i, 128)], wsem.at[1 + i]))
        raw_cps.append(pltpu.make_async_copy(wv_hbm.at[pl.ds(2048 * i, 2048)], wd.at[:, pl.ds(384 + 128 * i, 128)], wsem.at[4 + i]))
    for cp in raw_cps:
        cp.start()
    q_cps = [pltpu.make_async_copy(wq_hbm.at[h], wqkv.at[:, pl.ds(128 * h, 128)], wsem.at[7 + h]) for h in range(6)]
    for cp in q_cps:
        cp.start()
    wo_cp = pltpu.make_async_copy(wo_hbm, wo, wsem.at[13])
    wo_cp.start()
    wg_cp = pltpu.make_async_copy(wg_hbm, wg, wsem.at[14])
    wu_cp = pltpu.make_async_copy(wu_hbm, wu, wsem.at[15])
    wd_cp = pltpu.make_async_copy(wd_hbm, wd, wsem.at[16])
    wg_cp.start()
    wu_cp.start()

    ids = tok_row[...] - tp * VOCAB_LOCAL
    scale = jnp.where((ids >= 0) & (ids < VOCAB_LOCAL), NORMALIZER, 0.0).astype(F32)
    pos = pos_row[...]
    pos_hi = (pos >> 16).astype(F32)
    pos_lo = (pos & 65535).astype(F32)
    for k in range(2):
        cs = slice(128 * k, 128 * k + 128)
        scale_col[cs, :] = column_of(scale[:, cs])
        pos_col[cs, :] = column_of(pos_hi[:, cs]).astype(jnp.int32) * 65536 + column_of(pos_lo[:, cs]).astype(jnp.int32)

    def own(k):
        return pl.multiple_of(CHUNK * k + HALF * core, HALF)

    def theirs(k):
        return pl.multiple_of(CHUNK * k + HALF * (1 - core), HALF)

    def mine(f, k):
        return pl.multiple_of(CHUNK * f + HALF * k + QTR * core, QTR)

    def other(f, k):
        return pl.multiple_of(CHUNK * f + HALF * k + QTR * (1 - core), QTR)

    def e_d2d(k, j):
        return remote(part.at[pl.ds(theirs(k) + ROWP * j, ROWP)], rd.at[k, pl.ds(ROWP * j, ROWP)], esend.at[k, j], erecv.at[k, j], partner)

    def e_x(k, j):
        sl = pl.ds(ROWP * j, ROWP)
        return remote(ssum.at[k, sl], rxe.at[k, sl], exsend.at[k, j], exrecv.at[k, j], peer)

    def a_d2d(k, j):
        sl = pl.ds(own(k) + ROWP * j, ROWP)
        return remote(act.at[sl], act.at[sl], asend.at[k, j], arecv.at[k, j], partner)

    def a_in(k, j):
        sl = pl.ds(theirs(k) + ROWP * j, ROWP)
        return remote(act.at[sl], act.at[sl], asend.at[k, j], arecv.at[k, j], partner)

    def y_d2d(k, n):
        cs = pl.ds(COLP * n, COLP)
        return remote(part.at[pl.ds(theirs(k), HALF), cs], rd.at[k, :, cs], ysend.at[k, n], yrecv.at[k, n], partner)

    def y_x(k, f, n):
        sl, cs = pl.ds(QTR * f, QTR), pl.ds(COLP * n, COLP)
        return remote(ssum.at[k, sl, cs], rxy.at[k, sl, cs], yxsend.at[k, f, n], yxrecv.at[k, f, n], peer)

    def m_d2d(k, f, j):
        sl = pl.ds(mine(f, k) + ROWP * j, ROWP)
        return remote(act.at[sl], act.at[sl], msend.at[k, f, j], mrecv.at[k, f, j], partner)

    def m_in(k, f, j):
        sl = pl.ds(other(f, k) + ROWP * j, ROWP)
        return remote(act.at[sl], act.at[sl], msend.at[k, f, j], mrecv.at[k, f, j], partner)

    def z_d2d(f, k, n):
        cs = pl.ds(COLP * n, COLP)
        return remote(part.at[pl.ds(other(f, k), QTR), cs], rd.at[f, pl.ds(QTR * k, QTR), cs], zsend.at[f, k, n], zrecv.at[f, k, n], partner)

    def z_x(f, n):
        cs = pl.ds(COLP * n, COLP)
        return remote(ssum.at[f, pl.ds(pl.multiple_of(QTR * (1 - chip), QTR), QTR), cs], rxz.at[f, :, cs], zxsend.at[f, n], zxrecv.at[f, n], peer)

    def scale_rows(row):
        sl = pl.ds(row, ROWP)
        part[sl, :] = (part[sl, :].astype(F32) * scale_col[sl, :]).astype(BF)

    look_cp.wait()
    pl.semaphore_wait(barrier, 2)
    for k in range(2):
        for j in range(NRP):
            scale_rows(pl.multiple_of(theirs(k) + ROWP * j, ROWP))
            e_d2d(k, j).start()
    for k in range(2):
        for j in range(NRP):
            sl = pl.ds(ROWP * j, ROWP)
            row = pl.multiple_of(own(k) + ROWP * j, ROWP)
            scale_rows(row)
            e_d2d(k, j).wait_recv()
            ssum[k, sl, :] = part[pl.ds(row, ROWP), :] + rd[k, sl, :]
            e_x(k, j).start()

    for cp in raw_cps:
        cp.wait()
    for w in range(2):
        for i in range(3):
            def split_heads(b, carry, w=w, i=i):
                row = pl.multiple_of(b * 512, 512)
                f32buf[...] = wd[pl.ds(row, 512), pl.ds(384 * w + 128 * i, 128)].astype(F32)
                dst = pl.ds(pl.multiple_of(1024 * i + b * 256, 256), 256)
                for h in range(2):
                    wqkv[dst, pl.ds(768 + 256 * w + 128 * h, 128)] = f32buf[pl.ds(h, 256, stride=2), :].astype(BF)
                return carry
            lax.fori_loop(0, 4, split_heads, 0)
    wd_cp.start()

    gain1 = 1.0 + g1[...]
    gain2 = 1.0 + g2[...]
    gain3 = 1.0 + g3[...]
    gain4 = 1.0 + g4[...]

    def embed_chunk(k):
        for j in range(NRP):
            sl = pl.ds(ROWP * j, ROWP)
            e_x(k, j).wait_recv()
            emb = ssum[k, sl, :] + rxe[k, sl, :]
            resid[k, sl, :] = emb
            act[pl.ds(pl.multiple_of(own(k) + ROWP * j, ROWP), ROWP), :] = rms_rows(emb.astype(F32), gain1)
            a_d2d(k, j).start()
        for j in range(NRP):
            a_in(k, j).wait_recv()

    def qkv_chunk(k):
        rows = pl.ds(CHUNK * k, CHUNK)
        cos_c = cos_tab[rows, :]
        sin_c = sin_tab[rows, :]

        def rope(u):
            return u * cos_c + pltpu.roll(u, 64, 1) * sin_c

        for b in range(5):
            prod = jnp.dot(act[rows, :], wqkv[:, pl.ds(256 * b, 256)], preferred_element_type=F32)
            for h in range(2):
                u = prod[:, 128 * h:128 * h + 128]
                if b < 3:
                    qs[2 * b + h] = (rope(u) * QUERY_SCALE).astype(BF)
                elif b == 3:
                    ks[h, rows, :] = rope(u).astype(BF)
                else:
                    vs[h, rows, :] = u.astype(BF)

    def attend_chunk(k):
        span = CHUNK * (k + 1)
        offset = pos_col[pl.ds(CHUNK * k, CHUNK), :] - pos_row[:, pl.ds(0, span)]
        keep = (offset >= 0) & (offset < WINDOW)
        for g in range(2):
            kk = ks[g, pl.ds(0, span), :]
            vv = vs[g, pl.ds(0, span), :]
            for i in range(3):
                s = lax.dot_general(qs[3 * g + i], kk, (((1,), (1,)), ((), ())), preferred_element_type=F32)
                c = SOFT_CAP * jnp.tanh(s * (1.0 / SOFT_CAP))
                e = jnp.where(keep, jnp.exp(c), 0.0)
                pr = (e * (1.0 / jnp.sum(e, axis=-1, keepdims=True))).astype(BF)
                o = jnp.dot(pr, vv, preferred_element_type=F32)
                os_[:, pl.ds(128 * (3 * g + i), 128)] = o.astype(BF)

    def out_chunk(k):
        rows = pl.ds(CHUNK * k, CHUNK)
        for j in range(NRP):
            e_d2d(k, j).wait_send()
            e_x(k, j).wait_send()
            a_d2d(k, j).wait_send()

        def finish(n):
            cs = pl.ds(COLP * n, COLP)
            y_d2d(k, n).wait_recv()
            ssum[k, :, cs] = (part[pl.ds(own(k), HALF), cs].astype(F32) + rd[k, :, cs].astype(F32)).astype(BF)
            y_x(k, 0, n).start()

        for n in range(NCP):
            cs = pl.ds(COLP * n, COLP)
            part[rows, cs] = jnp.dot(os_[...], wo[:, cs], preferred_element_type=F32).astype(BF)
            y_d2d(k, n).start()
            if n > 0:
                finish(n - 1)
        finish(NCP - 1)
        for n in range(NCP):
            y_x(k, 1, n).start()

    def mid_block(k, f):
        for n in range(NCP):
            y_x(k, f, n).wait_recv()
        for j in range(QTR // ROWP):
            sl = pl.ds(QTR * f + ROWP * j, ROWP)
            y = (ssum[k, sl, :].astype(F32) + rxy[k, sl, :].astype(F32)).astype(BF).astype(F32)
            x1 = (resid[k, sl, :].astype(F32) + rms_rows(y, gain2).astype(F32)).astype(BF)
            resid[k, sl, :] = x1
            act[pl.ds(pl.multiple_of(mine(f, k) + ROWP * j, ROWP), ROWP), :] = rms_rows(x1.astype(F32), gain3)
            m_d2d(k, f, j).start()

    def mid_arrive(f):
        for k in range(2):
            for j in range(QTR // ROWP):
                m_in(k, f, j).wait_recv()

    def up_part(f, lo, hi):
        rows = pl.ds(CHUNK * f, CHUNK)

        def up(b, carry):
            cs = pl.ds(pl.multiple_of(UPB * b, UPB), UPB)
            gate = jnp.dot(act[rows, :], wg[:, cs], preferred_element_type=F32)
            upp = jnp.dot(act[rows, :], wu[:, cs], preferred_element_type=F32)
            hid[:, cs] = (jax.nn.gelu(gate, approximate=True) * upp).astype(BF)
            return carry
        lax.fori_loop(lo, hi, up, 0)

    def z_finish(f, n):
        cs = pl.ds(COLP * n, COLP)
        for k in range(2):
            z_d2d(f, k, n).wait_recv()
            sl = pl.ds(QTR * k, QTR)
            ssum[f, sl, cs] = (part[pl.ds(mine(f, k), QTR), cs].astype(F32) + rd[f, sl, cs].astype(F32)).astype(BF)
        z_x(f, n).start()

    def down_part(f):
        rows = pl.ds(CHUNK * f, CHUNK)
        for n in range(NCP):
            cs = pl.ds(COLP * n, COLP)
            part[rows, cs] = jnp.dot(hid[...], wd[:, cs], preferred_element_type=F32).astype(BF)
            for k in range(2):
                z_d2d(f, k, n).start()
            if n > 0:
                z_finish(f, n - 1)

    def output_rows(f):
        for n in range(NCP):
            z_x(f, n).wait_recv()
        keep_row = pl.multiple_of(QTR * chip, QTR)
        for j in range(QTR // ROWP):
            z = (ssum[f, pl.ds(keep_row + ROWP * j, ROWP), :].astype(F32) + rxz[f, pl.ds(ROWP * j, ROWP), :].astype(F32)).astype(BF).astype(F32)
            sl = pl.ds(QTR * f + ROWP * j, ROWP)
            out[0, sl, :] = (resid[chip, sl, :].astype(F32) + rms_rows(z, gain4).astype(F32)).astype(BF)

    embed_chunk(0)
    for cp in q_cps:
        cp.wait()
    qkv_chunk(0)
    attend_chunk(0)
    wo_cp.wait()
    out_chunk(0)
    embed_chunk(1)
    qkv_chunk(1)
    attend_chunk(1)
    out_chunk(1)
    mid_block(0, 0)
    mid_block(0, 1)
    wg_cp.wait()
    wu_cp.wait()
    wd_cp.wait()
    mid_block(1, 0)
    mid_arrive(0)
    up_part(0, 0, FFN // UPB)
    mid_block(1, 1)
    for k in range(2):
        for n in range(NCP):
            y_d2d(k, n).wait_send()
            for f in range(2):
                y_x(k, f, n).wait_send()
    down_part(0)
    mid_arrive(1)
    up_part(1, 0, 1)
    z_finish(0, NCP - 1)
    up_part(1, 1, FFN // UPB)
    down_part(1)
    z_finish(1, NCP - 1)
    output_rows(0)
    output_rows(1)
    for f in range(2):
        for k in range(2):
            for j in range(QTR // ROWP):
                m_d2d(k, f, j).wait_send()
            for n in range(NCP):
                z_d2d(f, k, n).wait_send()
        for n in range(NCP):
            z_x(f, n).wait_send()


def solution(mesh):
    in_specs = (P("dp", None), P("dp", None), P("tp", None), P(None, "tp", None), P(None, "tp", None), P(None, "tp", None), P("tp", None, None), P(None, "tp"), P(None, "tp"), P("tp", None), P(None), P(None), P(None), P(None))

    vm = pl.BlockSpec(memory_space=pltpu.VMEM)
    hb = pl.BlockSpec(memory_space=pl.ANY)
    dma = pltpu.SemaphoreType.DMA
    kernel = pl.pallas_call(
        layer_kernel,
        out_shape=jax.ShapeDtypeStruct((1, HALF, DIM), BF),
        in_specs=[hb, vm, vm, vm, vm] + [hb] * 7 + [vm] * 4,
        out_specs=vm,
        scratch_shapes=[
            pltpu.VMEM((DIM, 1280), BF),
            pltpu.VMEM((768, DIM), BF),
            pltpu.VMEM((DIM, FFN), BF),
            pltpu.VMEM((DIM, FFN), BF),
            pltpu.VMEM((FFN, DIM), BF),
            pltpu.VMEM((SEQ, DIM), BF),
            pltpu.VMEM((2, HALF, DIM), BF),
            pltpu.VMEM((2, HALF, DIM), BF),
            pltpu.VMEM((2, HALF, DIM), BF),
            pltpu.VMEM((2, HALF, DIM), BF),
            pltpu.VMEM((2, QTR, DIM), BF),
            pltpu.VMEM((SEQ, DIM), BF),
            pltpu.VMEM((2, HALF, DIM), BF),
            pltpu.VMEM((CHUNK, FFN), BF),
            pltpu.VMEM((6, CHUNK, 128), BF),
            pltpu.VMEM((2, SEQ, 128), BF),
            pltpu.VMEM((2, SEQ, 128), BF),
            pltpu.VMEM((CHUNK, 768), BF),
            pltpu.VMEM((512, 128), F32),
            pltpu.VMEM((SEQ, 1), F32),
            pltpu.VMEM((SEQ, 1), jnp.int32),
            dma((17,)),
            dma((2, NRP)), dma((2, NRP)),
            dma((2, NRP)), dma((2, NRP)),
            dma((2, NRP)), dma((2, NRP)),
            dma((2, NCP)), dma((2, NCP)),
            dma((2, 2, NCP)), dma((2, 2, NCP)),
            dma((2, 2, QTR // ROWP)), dma((2, 2, QTR // ROWP)),
            dma((2, 2, NCP)), dma((2, 2, NCP)),
            dma((2, NCP)), dma((2, NCP)),
        ],
        compiler_params=pltpu.CompilerParams(collective_id=0, has_side_effects=True, vmem_limit_bytes=67043328),
        name="decoder_layer",
    )

    def device_step(tokens, positions, embed_block, w_query, w_key, w_value, w_out, w_gate, w_up, w_down, g1, g2, g3, g4):
        dev_rank = lax.axis_index("tp")
        vocab_local, model_dim = embed_block.shape
        ids = tokens[0] - dev_rank * vocab_local
        in_block = (ids >= 0) & (ids < vocab_local)
        spread = jnp.arange(SEQ, dtype=jnp.int32) * (vocab_local // SEQ)
        looked = jnp.take(embed_block, jnp.where(in_block, ids, spread), axis=0, mode="clip")
        half = jnp.arange(128, dtype=jnp.int32) % 64
        inv_freq = ROPE_BASE ** (-2.0 * half.astype(F32) / 128)
        angles = positions[0].astype(F32)[:, None] * inv_freq
        cos_tab = jnp.cos(angles)
        sin_tab = jnp.sin(angles) * jnp.where(jnp.arange(128) < 64, -1.0, 1.0).astype(F32)
        return kernel(looked, tokens, positions, cos_tab, sin_tab,
                      w_query.transpose(1, 0, 2), w_key.reshape(2 * model_dim, 128), w_value.reshape(2 * model_dim, 128), w_out.reshape(768, model_dim),
                      w_gate, w_up, w_down, g1[None], g2[None], g3[None], g4[None])

    return jax.shard_map(device_step, mesh=mesh, in_specs=in_specs, out_specs=P("dp", "tp", None), check_vma=False)
```

```python
import functools

import jax
import jax.numpy as jnp
import numpy as np
from jax import lax
from jax.experimental import pallas as pl
from jax.experimental.pallas import tpu as pltpu
from jax.sharding import PartitionSpec as P

WINDOW = 4096
QUERY_SCALE = 256.0 ** -0.5
SOFT_CAP = 50.0
NORM_EPS = 1e-6
ROPE_BASE = 10000.0
SEQ = 256
DIM = 3072
FFN = 2048
CHUNK = 128
HALF = 64
QTR = 32
UPB = 512
VOCAB_LOCAL = 32064
NORMALIZER = float(np.asarray(np.sqrt(np.float32(DIM)), dtype=jnp.bfloat16))
ROWP = 16
NRP = HALF // ROWP
COLP = 1024
NCP = DIM // COLP
BF = jnp.bfloat16
F32 = jnp.float32


def rms_rows(u, gain):
    mean_sq = jnp.mean(u * u, axis=-1, keepdims=True)
    return (u * lax.rsqrt(mean_sq + NORM_EPS) * gain).astype(BF)


def column_of(row_f32):
    diag = lax.broadcasted_iota(jnp.int32, (128, 128), 0) == lax.broadcasted_iota(jnp.int32, (128, 128), 1)
    return jnp.sum(jnp.where(diag, jnp.broadcast_to(row_f32, (128, 128)), 0.0), axis=1, keepdims=True)


def layer_kernel(looked, tok_row, pos_row, cos_tab, sin_tab, wq_hbm, wk_hbm, wv_hbm, wo_hbm, wg_hbm, wu_hbm, wd_hbm, g1, g2, g3, g4,
                 out,
                 wqkv, wo, wg, wu, wd, part, ssum, rd, rxe, rxy, rxz, act, resid, hid, qs, ks, vs, os_, f32buf, scale_col, pos_col,
                 wsem, esend, erecv, exsend, exrecv, asend, arecv, ysend, yrecv, yxsend, yxrecv, msend, mrecv, zsend, zrecv, zxsend, zxrecv):
    tp = lax.axis_index("tp")
    chip = tp // 2
    core = tp % 2
    partner = chip * 2 + (1 - core)
    peer = (1 - chip) * 2 + core

    def remote(src, dst, ssem, rsem, dev):
        return pltpu.make_async_remote_copy(src_ref=src, dst_ref=dst, send_sem=ssem, recv_sem=rsem, device_id={"tp": dev}, device_id_type=pl.DeviceIdType.MESH)

    barrier = pltpu.get_barrier_semaphore()
    for dev in (partner, peer):
        pl.semaphore_signal(barrier, inc=1, device_id={"tp": dev}, device_id_type=pl.DeviceIdType.MESH)

    look_cp = pltpu.make_async_copy(looked, part, wsem.at[0])
    look_cp.start()
    raw_cps = []
    for i in range(3):
        raw_cps.append(pltpu.make_async_copy(wk_hbm.at[pl.ds(2048 * i, 2048)], wd.at[:, pl.ds(128 * i, 128)], wsem.at[1 + i]))
        raw_cps.append(pltpu.make_async_copy(wv_hbm.at[pl.ds(2048 * i, 2048)], wd.at[:, pl.ds(384 + 128 * i, 128)], wsem.at[4 + i]))
    q_cps = [pltpu.make_async_copy(wq_hbm.at[h], wqkv.at[:, pl.ds(128 * h, 128)], wsem.at[7 + h]) for h in range(6)]
    wo_cp = pltpu.make_async_copy(wo_hbm, wo, wsem.at[13])
    wg_cp = pltpu.make_async_copy(wg_hbm, wg, wsem.at[14])
    wu_cp = pltpu.make_async_copy(wu_hbm, wu, wsem.at[15])
    wd_cp = pltpu.make_async_copy(wd_hbm, wd, wsem.at[16])

    ids = tok_row[...] - tp * VOCAB_LOCAL
    scale = jnp.where((ids >= 0) & (ids < VOCAB_LOCAL), NORMALIZER, 0.0).astype(F32)
    pos = pos_row[...]
    pos_hi = (pos >> 16).astype(F32)
    pos_lo = (pos & 65535).astype(F32)
    for k in range(2):
        cs = slice(128 * k, 128 * k + 128)
        scale_col[cs, :] = column_of(scale[:, cs])
        pos_col[cs, :] = column_of(pos_hi[:, cs]).astype(jnp.int32) * 65536 + column_of(pos_lo[:, cs]).astype(jnp.int32)

    def own(k):
        return pl.multiple_of(CHUNK * k + HALF * core, HALF)

    def theirs(k):
        return pl.multiple_of(CHUNK * k + HALF * (1 - core), HALF)

    def mine(f, k):
        return pl.multiple_of(CHUNK * f + HALF * k + QTR * core, QTR)

    def other(f, k):
        return pl.multiple_of(CHUNK * f + HALF * k + QTR * (1 - core), QTR)

    def e_d2d(k, j):
        return remote(part.at[pl.ds(theirs(k) + ROWP * j, ROWP)], rd.at[k, pl.ds(ROWP * j, ROWP)], esend.at[k, j], erecv.at[k, j], partner)

    def e_x(k, j):
        sl = pl.ds(ROWP * j, ROWP)
        return remote(ssum.at[k, sl], rxe.at[k, sl], exsend.at[k, j], exrecv.at[k, j], peer)

    def a_d2d(k, j):
        sl = pl.ds(own(k) + ROWP * j, ROWP)
        return remote(act.at[sl], act.at[sl], asend.at[k, j], arecv.at[k, j], partner)

    def a_in(k, j):
        sl = pl.ds(theirs(k) + ROWP * j, ROWP)
        return remote(act.at[sl], act.at[sl], asend.at[k, j], arecv.at[k, j], partner)

    def y_d2d(k, n):
        cs = pl.ds(COLP * n, COLP)
        return remote(part.at[pl.ds(theirs(k), HALF), cs], rd.at[k, :, cs], ysend.at[k, n], yrecv.at[k, n], partner)

    def y_x(k, f, n):
        sl, cs = pl.ds(QTR * f, QTR), pl.ds(COLP * n, COLP)
        return remote(ssum.at[k, sl, cs], rxy.at[k, sl, cs], yxsend.at[k, f, n], yxrecv.at[k, f, n], peer)

    def m_d2d(k, f, j):
        sl = pl.ds(mine(f, k) + ROWP * j, ROWP)
        return remote(act.at[sl], act.at[sl], msend.at[k, f, j], mrecv.at[k, f, j], partner)

    def m_in(k, f, j):
        sl = pl.ds(other(f, k) + ROWP * j, ROWP)
        return remote(act.at[sl], act.at[sl], msend.at[k, f, j], mrecv.at[k, f, j], partner)

    def z_d2d(f, k, n):
        cs = pl.ds(COLP * n, COLP)
        return remote(part.at[pl.ds(other(f, k), QTR), cs], rd.at[f, pl.ds(QTR * k, QTR), cs], zsend.at[f, k, n], zrecv.at[f, k, n], partner)

    def z_x(f, n):
        cs = pl.ds(COLP * n, COLP)
        return remote(ssum.at[f, pl.ds(pl.multiple_of(QTR * (1 - chip), QTR), QTR), cs], rxz.at[f, :, cs], zxsend.at[f, n], zxrecv.at[f, n], peer)

    def scale_rows(row):
        sl = pl.ds(row, ROWP)
        part[sl, :] = (part[sl, :].astype(F32) * scale_col[sl, :]).astype(BF)

    look_cp.wait()
    pl.semaphore_wait(barrier, 2)
    for k in range(2):
        for j in range(NRP):
            scale_rows(pl.multiple_of(theirs(k) + ROWP * j, ROWP))
            e_d2d(k, j).start()
    for cp in raw_cps + q_cps:
        cp.start()
    for k in range(2):
        for j in range(NRP):
            sl = pl.ds(ROWP * j, ROWP)
            row = pl.multiple_of(own(k) + ROWP * j, ROWP)
            scale_rows(row)
            e_d2d(k, j).wait_recv()
            ssum[k, sl, :] = part[pl.ds(row, ROWP), :] + rd[k, sl, :]
            e_x(k, j).start()

    for cp in raw_cps:
        cp.wait()
    for w in range(2):
        for i in range(3):
            def split_heads(b, carry, w=w, i=i):
                row = pl.multiple_of(b * 512, 512)
                f32buf[...] = wd[pl.ds(row, 512), pl.ds(384 * w + 128 * i, 128)].astype(F32)
                dst = pl.ds(pl.multiple_of(1024 * i + b * 256, 256), 256)
                for h in range(2):
                    wqkv[dst, pl.ds(768 + 256 * w + 128 * h, 128)] = f32buf[pl.ds(h, 256, stride=2), :].astype(BF)
                return carry
            lax.fori_loop(0, 4, split_heads, 0)
    wo_cp.start()

    gain1 = 1.0 + g1[...]
    gain2 = 1.0 + g2[...]
    gain3 = 1.0 + g3[...]
    gain4 = 1.0 + g4[...]

    def embed_chunk(k):
        for j in range(NRP):
            sl = pl.ds(ROWP * j, ROWP)
            e_x(k, j).wait_recv()
            emb = ssum[k, sl, :] + rxe[k, sl, :]
            resid[k, sl, :] = emb
            act[pl.ds(pl.multiple_of(own(k) + ROWP * j, ROWP), ROWP), :] = rms_rows(emb.astype(F32), gain1)
            a_d2d(k, j).start()
        for j in range(NRP):
            a_in(k, j).wait_recv()

    def qkv_chunk(k):
        rows = pl.ds(CHUNK * k, CHUNK)
        cos_c = cos_tab[rows, :]
        sin_c = sin_tab[rows, :]

        def rope(u):
            return u * cos_c + pltpu.roll(u, 64, 1) * sin_c

        for b in range(5):
            prod = jnp.dot(act[rows, :], wqkv[:, pl.ds(256 * b, 256)], preferred_element_type=F32)
            for h in range(2):
                u = prod[:, 128 * h:128 * h + 128]
                if b < 3:
                    qs[2 * b + h] = (rope(u) * QUERY_SCALE).astype(BF)
                elif b == 3:
                    ks[h, rows, :] = rope(u).astype(BF)
                else:
                    vs[h, rows, :] = u.astype(BF)

    def attend_chunk(k):
        span = CHUNK * (k + 1)
        offset = pos_col[pl.ds(CHUNK * k, CHUNK), :] - pos_row[:, pl.ds(0, span)]
        keep = (offset >= 0) & (offset < WINDOW)
        for g in range(2):
            kk = ks[g, pl.ds(0, span), :]
            vv = vs[g, pl.ds(0, span), :]
            for i in range(3):
                s = lax.dot_general(qs[3 * g + i], kk, (((1,), (1,)), ((), ())), preferred_element_type=F32)
                c = SOFT_CAP * jnp.tanh(s * (1.0 / SOFT_CAP))
                e = jnp.where(keep, jnp.exp(c), 0.0)
                pr = (e * (1.0 / jnp.sum(e, axis=-1, keepdims=True))).astype(BF)
                o = jnp.dot(pr, vv, preferred_element_type=F32)
                os_[:, pl.ds(128 * (3 * g + i), 128)] = o.astype(BF)

    def out_chunk(k):
        rows = pl.ds(CHUNK * k, CHUNK)
        for j in range(NRP):
            e_d2d(k, j).wait_send()
            e_x(k, j).wait_send()
            a_d2d(k, j).wait_send()

        def finish(n):
            cs = pl.ds(COLP * n, COLP)
            y_d2d(k, n).wait_recv()
            ssum[k, :, cs] = (part[pl.ds(own(k), HALF), cs].astype(F32) + rd[k, :, cs].astype(F32)).astype(BF)
            y_x(k, 0, n).start()

        for n in range(NCP):
            cs = pl.ds(COLP * n, COLP)
            part[rows, cs] = jnp.dot(os_[...], wo[:, cs], preferred_element_type=F32).astype(BF)
            y_d2d(k, n).start()
            if n > 0:
                finish(n - 1)
        finish(NCP - 1)
        for n in range(NCP):
            y_x(k, 1, n).start()

    def mid_block(k, f):
        for n in range(NCP):
            y_x(k, f, n).wait_recv()
        for j in range(QTR // ROWP):
            sl = pl.ds(QTR * f + ROWP * j, ROWP)
            y = (ssum[k, sl, :].astype(F32) + rxy[k, sl, :].astype(F32)).astype(BF).astype(F32)
            x1 = (resid[k, sl, :].astype(F32) + rms_rows(y, gain2).astype(F32)).astype(BF)
            resid[k, sl, :] = x1
            act[pl.ds(pl.multiple_of(mine(f, k) + ROWP * j, ROWP), ROWP), :] = rms_rows(x1.astype(F32), gain3)
            m_d2d(k, f, j).start()

    def mid_arrive(f):
        for k in range(2):
            for j in range(QTR // ROWP):
                m_in(k, f, j).wait_recv()

    def up_part(f, lo, hi):
        rows = pl.ds(CHUNK * f, CHUNK)

        def up(b, carry):
            cs = pl.ds(pl.multiple_of(UPB * b, UPB), UPB)
            gate = jnp.dot(act[rows, :], wg[:, cs], preferred_element_type=F32)
            upp = jnp.dot(act[rows, :], wu[:, cs], preferred_element_type=F32)
            hid[:, cs] = (jax.nn.gelu(gate, approximate=True) * upp).astype(BF)
            return carry
        lax.fori_loop(lo, hi, up, 0)

    def z_finish(f, n):
        cs = pl.ds(COLP * n, COLP)
        for k in range(2):
            z_d2d(f, k, n).wait_recv()
            sl = pl.ds(QTR * k, QTR)
            ssum[f, sl, cs] = (part[pl.ds(mine(f, k), QTR), cs].astype(F32) + rd[f, sl, cs].astype(F32)).astype(BF)
        z_x(f, n).start()

    def down_part(f):
        rows = pl.ds(CHUNK * f, CHUNK)
        for n in range(NCP):
            cs = pl.ds(COLP * n, COLP)
            part[rows, cs] = jnp.dot(hid[...], wd[:, cs], preferred_element_type=F32).astype(BF)
            for k in range(2):
                z_d2d(f, k, n).start()
            if n > 0:
                z_finish(f, n - 1)

    def output_rows(f):
        for n in range(NCP):
            z_x(f, n).wait_recv()
        keep_row = pl.multiple_of(QTR * chip, QTR)
        for j in range(QTR // ROWP):
            z = (ssum[f, pl.ds(keep_row + ROWP * j, ROWP), :].astype(F32) + rxz[f, pl.ds(ROWP * j, ROWP), :].astype(F32)).astype(BF).astype(F32)
            sl = pl.ds(QTR * f + ROWP * j, ROWP)
            out[0, sl, :] = (resid[chip, sl, :].astype(F32) + rms_rows(z, gain4).astype(F32)).astype(BF)

    embed_chunk(0)
    wg_cp.start()
    wu_cp.start()
    for cp in q_cps:
        cp.wait()
    qkv_chunk(0)
    attend_chunk(0)
    wo_cp.wait()
    out_chunk(0)
    wd_cp.start()
    embed_chunk(1)
    qkv_chunk(1)
    attend_chunk(1)
    out_chunk(1)
    mid_block(0, 0)
    mid_block(0, 1)
    wg_cp.wait()
    wu_cp.wait()
    wd_cp.wait()
    mid_block(1, 0)
    mid_arrive(0)
    up_part(0, 0, FFN // UPB)
    mid_block(1, 1)
    for k in range(2):
        for n in range(NCP):
            y_d2d(k, n).wait_send()
            for f in range(2):
                y_x(k, f, n).wait_send()
    down_part(0)
    mid_arrive(1)
    up_part(1, 0, 1)
    z_finish(0, NCP - 1)
    up_part(1, 1, FFN // UPB)
    down_part(1)
    z_finish(1, NCP - 1)
    output_rows(0)
    output_rows(1)
    for f in range(2):
        for k in range(2):
            for j in range(QTR // ROWP):
                m_d2d(k, f, j).wait_send()
            for n in range(NCP):
                z_d2d(f, k, n).wait_send()
        for n in range(NCP):
            z_x(f, n).wait_send()


def solution(mesh):
    in_specs = (P("dp", None), P("dp", None), P("tp", None), P(None, "tp", None), P(None, "tp", None), P(None, "tp", None), P("tp", None, None), P(None, "tp"), P(None, "tp"), P("tp", None), P(None), P(None), P(None), P(None))

    vm = pl.BlockSpec(memory_space=pltpu.VMEM)
    hb = pl.BlockSpec(memory_space=pl.ANY)
    dma = pltpu.SemaphoreType.DMA
    kernel = pl.pallas_call(
        layer_kernel,
        out_shape=jax.ShapeDtypeStruct((1, HALF, DIM), BF),
        in_specs=[hb, vm, vm, vm, vm] + [hb] * 7 + [vm] * 4,
        out_specs=vm,
        scratch_shapes=[
            pltpu.VMEM((DIM, 1280), BF),
            pltpu.VMEM((768, DIM), BF),
            pltpu.VMEM((DIM, FFN), BF),
            pltpu.VMEM((DIM, FFN), BF),
            pltpu.VMEM((FFN, DIM), BF),
            pltpu.VMEM((SEQ, DIM), BF),
            pltpu.VMEM((2, HALF, DIM), BF),
            pltpu.VMEM((2, HALF, DIM), BF),
            pltpu.VMEM((2, HALF, DIM), BF),
            pltpu.VMEM((2, HALF, DIM), BF),
            pltpu.VMEM((2, QTR, DIM), BF),
            pltpu.VMEM((SEQ, DIM), BF),
            pltpu.VMEM((2, HALF, DIM), BF),
            pltpu.VMEM((CHUNK, FFN), BF),
            pltpu.VMEM((6, CHUNK, 128), BF),
            pltpu.VMEM((2, SEQ, 128), BF),
            pltpu.VMEM((2, SEQ, 128), BF),
            pltpu.VMEM((CHUNK, 768), BF),
            pltpu.VMEM((512, 128), F32),
            pltpu.VMEM((SEQ, 1), F32),
            pltpu.VMEM((SEQ, 1), jnp.int32),
            dma((17,)),
            dma((2, NRP)), dma((2, NRP)),
            dma((2, NRP)), dma((2, NRP)),
            dma((2, NRP)), dma((2, NRP)),
            dma((2, NCP)), dma((2, NCP)),
            dma((2, 2, NCP)), dma((2, 2, NCP)),
            dma((2, 2, QTR // ROWP)), dma((2, 2, QTR // ROWP)),
            dma((2, 2, NCP)), dma((2, 2, NCP)),
            dma((2, NCP)), dma((2, NCP)),
        ],
        compiler_params=pltpu.CompilerParams(collective_id=0, has_side_effects=True, vmem_limit_bytes=67043328),
        name="decoder_layer",
    )

    def device_step(tokens, positions, embed_block, w_query, w_key, w_value, w_out, w_gate, w_up, w_down, g1, g2, g3, g4):
        dev_rank = lax.axis_index("tp")
        vocab_local, model_dim = embed_block.shape
        ids = tokens[0] - dev_rank * vocab_local
        in_block = (ids >= 0) & (ids < vocab_local)
        spread = jnp.arange(SEQ, dtype=jnp.int32) * (vocab_local // SEQ)
        looked = jnp.take(embed_block, jnp.where(in_block, ids, spread), axis=0, mode="clip")
        half = jnp.arange(128, dtype=jnp.int32) % 64
        inv_freq = ROPE_BASE ** (-2.0 * half.astype(F32) / 128)
        angles = positions[0].astype(F32)[:, None] * inv_freq
        cos_tab = jnp.cos(angles)
        sin_tab = jnp.sin(angles) * jnp.where(jnp.arange(128) < 64, -1.0, 1.0).astype(F32)
        return kernel(looked, tokens, positions, cos_tab, sin_tab,
                      w_query.transpose(1, 0, 2), w_key.reshape(2 * model_dim, 128), w_value.reshape(2 * model_dim, 128), w_out.reshape(768, model_dim),
                      w_gate, w_up, w_down, g1[None], g2[None], g3[None], g4[None])

    return jax.shard_map(device_step, mesh=mesh, in_specs=in_specs, out_specs=P("dp", "tp", None), check_vma=False)
```

```python
import functools

import jax
import jax.numpy as jnp
import numpy as np
from jax import lax
from jax.experimental import pallas as pl
from jax.experimental.pallas import tpu as pltpu
from jax.sharding import PartitionSpec as P

WINDOW = 4096
QUERY_SCALE = 256.0 ** -0.5
SOFT_CAP = 50.0
NORM_EPS = 1e-6
ROPE_BASE = 10000.0
SEQ = 256
DIM = 3072
FFN = 2048
CHUNK = 128
HALF = 64
QTR = 32
UPB = 512
VOCAB_LOCAL = 32064
NORMALIZER = float(np.asarray(np.sqrt(np.float32(DIM)), dtype=jnp.bfloat16))
ROWP = 16
NRP = HALF // ROWP
COLP = 1024
NCP = DIM // COLP
BF = jnp.bfloat16
F32 = jnp.float32


def rms_rows(u, gain):
    mean_sq = jnp.mean(u * u, axis=-1, keepdims=True)
    return (u * lax.rsqrt(mean_sq + NORM_EPS) * gain).astype(BF)


def column_of(row_f32):
    diag = lax.broadcasted_iota(jnp.int32, (128, 128), 0) == lax.broadcasted_iota(jnp.int32, (128, 128), 1)
    return jnp.sum(jnp.where(diag, jnp.broadcast_to(row_f32, (128, 128)), 0.0), axis=1, keepdims=True)


def layer_kernel(looked, tok_row, pos_row, cos_tab, sin_tab, wq_hbm, wk_hbm, wv_hbm, wo_hbm, wg_hbm, wu_hbm, wd_hbm, g1, g2, g3, g4,
                 out,
                 wqkv, wo, wg, wu, wd, part, ssum, rd, rxe, rxy, rxz, act, resid, hid, qs, ks, vs, os_, f32buf, scale_col, pos_col,
                 wsem, esend, erecv, exsend, exrecv, asend, arecv, ysend, yrecv, yxsend, yxrecv, msend, mrecv, zsend, zrecv, zxsend, zxrecv):
    tp = lax.axis_index("tp")
    chip = tp // 2
    core = tp % 2
    partner = chip * 2 + (1 - core)
    peer = (1 - chip) * 2 + core

    def remote(src, dst, ssem, rsem, dev):
        return pltpu.make_async_remote_copy(src_ref=src, dst_ref=dst, send_sem=ssem, recv_sem=rsem, device_id={"tp": dev}, device_id_type=pl.DeviceIdType.MESH)

    barrier = pltpu.get_barrier_semaphore()
    for dev in (partner, peer):
        pl.semaphore_signal(barrier, inc=1, device_id={"tp": dev}, device_id_type=pl.DeviceIdType.MESH)

    look_cp = pltpu.make_async_copy(looked, part, wsem.at[0])
    look_cp.start()
    raw_cps = []
    for i in range(3):
        raw_cps.append(pltpu.make_async_copy(wk_hbm.at[pl.ds(2048 * i, 2048)], wd.at[:, pl.ds(128 * i, 128)], wsem.at[1 + i]))
        raw_cps.append(pltpu.make_async_copy(wv_hbm.at[pl.ds(2048 * i, 2048)], wd.at[:, pl.ds(384 + 128 * i, 128)], wsem.at[4 + i]))
    q_cps = [pltpu.make_async_copy(wq_hbm.at[h], wqkv.at[:, pl.ds(128 * h, 128)], wsem.at[7 + h]) for h in range(6)]
    wo_cp = pltpu.make_async_copy(wo_hbm, wo, wsem.at[13])
    wg_cp = pltpu.make_async_copy(wg_hbm, wg, wsem.at[14])
    wu_cp = pltpu.make_async_copy(wu_hbm, wu, wsem.at[15])
    wd_cp = pltpu.make_async_copy(wd_hbm, wd, wsem.at[16])

    ids = tok_row[...] - tp * VOCAB_LOCAL
    scale = jnp.where((ids >= 0) & (ids < VOCAB_LOCAL), NORMALIZER, 0.0).astype(F32)
    pos = pos_row[...]
    pos_hi = (pos >> 16).astype(F32)
    pos_lo = (pos & 65535).astype(F32)
    for k in range(2):
        cs = slice(128 * k, 128 * k + 128)
        scale_col[cs, :] = column_of(scale[:, cs])
        pos_col[cs, :] = column_of(pos_hi[:, cs]).astype(jnp.int32) * 65536 + column_of(pos_lo[:, cs]).astype(jnp.int32)

    def own(k):
        return pl.multiple_of(CHUNK * k + HALF * core, HALF)

    def theirs(k):
        return pl.multiple_of(CHUNK * k + HALF * (1 - core), HALF)

    def mine(f, k):
        return pl.multiple_of(CHUNK * f + HALF * k + QTR * core, QTR)

    def other(f, k):
        return pl.multiple_of(CHUNK * f + HALF * k + QTR * (1 - core), QTR)

    def e_d2d(k, j):
        return remote(part.at[pl.ds(theirs(k) + ROWP * j, ROWP)], rd.at[k, pl.ds(ROWP * j, ROWP)], esend.at[k, j], erecv.at[k, j], partner)

    def e_x(k, j):
        sl = pl.ds(QTR * j, QTR)
        return remote(ssum.at[k, sl], rxe.at[k, sl], exsend.at[k, j], exrecv.at[k, j], peer)

    def a_d2d(k, j):
        sl = pl.ds(own(k) + ROWP * j, ROWP)
        return remote(act.at[sl], act.at[sl], asend.at[k, j], arecv.at[k, j], partner)

    def a_in(k, j):
        sl = pl.ds(theirs(k) + ROWP * j, ROWP)
        return remote(act.at[sl], act.at[sl], asend.at[k, j], arecv.at[k, j], partner)

    def y_d2d(k, n):
        cs = pl.ds(COLP * n, COLP)
        return remote(part.at[pl.ds(theirs(k), HALF), cs], rd.at[k, :, cs], ysend.at[k, n], yrecv.at[k, n], partner)

    def y_x(k, f):
        sl = pl.ds(QTR * f, QTR)
        return remote(ssum.at[k, sl], rxy.at[k, sl], yxsend.at[k, f], yxrecv.at[k, f], peer)

    def m_d2d(k, f, j):
        sl = pl.ds(mine(f, k) + ROWP * j, ROWP)
        return remote(act.at[sl], act.at[sl], msend.at[k, f, j], mrecv.at[k, f, j], partner)

    def m_in(k, f, j):
        sl = pl.ds(other(f, k) + ROWP * j, ROWP)
        return remote(act.at[sl], act.at[sl], msend.at[k, f, j], mrecv.at[k, f, j], partner)

    def z_d2d(f, k, n):
        cs = pl.ds(COLP * n, COLP)
        return remote(part.at[pl.ds(other(f, k), QTR), cs], rd.at[f, pl.ds(QTR * k, QTR), cs], zsend.at[f, k, n], zrecv.at[f, k, n], partner)

    def z_x(f, n):
        cs = pl.ds(COLP * n, COLP)
        return remote(ssum.at[f, pl.ds(pl.multiple_of(QTR * (1 - chip), QTR), QTR), cs], rxz.at[f, :, cs], zxsend.at[f, n], zxrecv.at[f, n], peer)

    def scale_rows(row):
        sl = pl.ds(row, ROWP)
        part[sl, :] = (part[sl, :].astype(F32) * scale_col[sl, :]).astype(BF)

    look_cp.wait()
    pl.semaphore_wait(barrier, 2)
    for k in range(2):
        for j in range(NRP):
            scale_rows(pl.multiple_of(theirs(k) + ROWP * j, ROWP))
            e_d2d(k, j).start()
    for cp in raw_cps + q_cps:
        cp.start()
    for k in range(2):
        for j in range(NRP):
            sl = pl.ds(ROWP * j, ROWP)
            row = pl.multiple_of(own(k) + ROWP * j, ROWP)
            scale_rows(row)
            e_d2d(k, j).wait_recv()
            ssum[k, sl, :] = part[pl.ds(row, ROWP), :] + rd[k, sl, :]
            if j % 2 == 1:
                e_x(k, j // 2).start()

    for cp in raw_cps:
        cp.wait()
    for w in range(2):
        for i in range(3):
            def split_heads(b, carry, w=w, i=i):
                row = pl.multiple_of(b * 512, 512)
                f32buf[...] = wd[pl.ds(row, 512), pl.ds(384 * w + 128 * i, 128)].astype(F32)
                dst = pl.ds(pl.multiple_of(1024 * i + b * 256, 256), 256)
                for h in range(2):
                    wqkv[dst, pl.ds(768 + 256 * w + 128 * h, 128)] = f32buf[pl.ds(h, 256, stride=2), :].astype(BF)
                return carry
            lax.fori_loop(0, 4, split_heads, 0)
    wo_cp.start()

    gain1 = 1.0 + g1[...]
    gain2 = 1.0 + g2[...]
    gain3 = 1.0 + g3[...]
    gain4 = 1.0 + g4[...]

    def embed_chunk(k):
        for j in range(NRP):
            sl = pl.ds(ROWP * j, ROWP)
            if j % 2 == 0:
                e_x(k, j // 2).wait_recv()
            emb = ssum[k, sl, :] + rxe[k, sl, :]
            resid[k, sl, :] = emb
            act[pl.ds(pl.multiple_of(own(k) + ROWP * j, ROWP), ROWP), :] = rms_rows(emb.astype(F32), gain1)
            a_d2d(k, j).start()
        for j in range(NRP):
            a_in(k, j).wait_recv()

    def qkv_chunk(k):
        rows = pl.ds(CHUNK * k, CHUNK)
        cos_c = cos_tab[rows, :]
        sin_c = sin_tab[rows, :]

        def rope(u):
            return u * cos_c + pltpu.roll(u, 64, 1) * sin_c

        for b in range(5):
            prod = jnp.dot(act[rows, :], wqkv[:, pl.ds(256 * b, 256)], preferred_element_type=F32)
            for h in range(2):
                u = prod[:, 128 * h:128 * h + 128]
                if b < 3:
                    qs[2 * b + h] = (rope(u) * QUERY_SCALE).astype(BF)
                elif b == 3:
                    ks[h, rows, :] = rope(u).astype(BF)
                else:
                    vs[h, rows, :] = u.astype(BF)

    def attend_chunk(k):
        span = CHUNK * (k + 1)
        offset = pos_col[pl.ds(CHUNK * k, CHUNK), :] - pos_row[:, pl.ds(0, span)]
        keep = (offset >= 0) & (offset < WINDOW)
        for g in range(2):
            kk = ks[g, pl.ds(0, span), :]
            vv = vs[g, pl.ds(0, span), :]
            for i in range(3):
                s = lax.dot_general(qs[3 * g + i], kk, (((1,), (1,)), ((), ())), preferred_element_type=F32)
                c = SOFT_CAP * jnp.tanh(s * (1.0 / SOFT_CAP))
                e = jnp.where(keep, jnp.exp(c), 0.0)
                pr = (e * (1.0 / jnp.sum(e, axis=-1, keepdims=True))).astype(BF)
                o = jnp.dot(pr, vv, preferred_element_type=F32)
                os_[:, pl.ds(128 * (3 * g + i), 128)] = o.astype(BF)

    def out_chunk(k):
        rows = pl.ds(CHUNK * k, CHUNK)
        for j in range(NRP):
            e_d2d(k, j).wait_send()
            if j % 2 == 0:
                e_x(k, j // 2).wait_send()
            a_d2d(k, j).wait_send()

        def finish(n):
            cs = pl.ds(COLP * n, COLP)
            y_d2d(k, n).wait_recv()
            ssum[k, :, cs] = (part[pl.ds(own(k), HALF), cs].astype(F32) + rd[k, :, cs].astype(F32)).astype(BF)

        for n in range(NCP):
            cs = pl.ds(COLP * n, COLP)
            part[rows, cs] = jnp.dot(os_[...], wo[:, cs], preferred_element_type=F32).astype(BF)
            y_d2d(k, n).start()
            if n > 0:
                finish(n - 1)
        finish(NCP - 1)
        for f in range(2):
            y_x(k, f).start()

    def mid_block(k, f):
        y_x(k, f).wait_recv()
        for j in range(QTR // ROWP):
            sl = pl.ds(QTR * f + ROWP * j, ROWP)
            y = (ssum[k, sl, :].astype(F32) + rxy[k, sl, :].astype(F32)).astype(BF).astype(F32)
            x1 = (resid[k, sl, :].astype(F32) + rms_rows(y, gain2).astype(F32)).astype(BF)
            resid[k, sl, :] = x1
            act[pl.ds(pl.multiple_of(mine(f, k) + ROWP * j, ROWP), ROWP), :] = rms_rows(x1.astype(F32), gain3)
            m_d2d(k, f, j).start()

    def mid_arrive(f):
        for k in range(2):
            for j in range(QTR // ROWP):
                m_in(k, f, j).wait_recv()

    def up_part(f, lo, hi):
        rows = pl.ds(CHUNK * f, CHUNK)

        def up(b, carry):
            cs = pl.ds(pl.multiple_of(UPB * b, UPB), UPB)
            gate = jnp.dot(act[rows, :], wg[:, cs], preferred_element_type=F32)
            upp = jnp.dot(act[rows, :], wu[:, cs], preferred_element_type=F32)
            hid[:, cs] = (jax.nn.gelu(gate, approximate=True) * upp).astype(BF)
            return carry
        lax.fori_loop(lo, hi, up, 0)

    def z_finish(f, n):
        cs = pl.ds(COLP * n, COLP)
        for k in range(2):
            z_d2d(f, k, n).wait_recv()
            sl = pl.ds(QTR * k, QTR)
            ssum[f, sl, cs] = (part[pl.ds(mine(f, k), QTR), cs].astype(F32) + rd[f, sl, cs].astype(F32)).astype(BF)
        z_x(f, n).start()

    def down_part(f):
        rows = pl.ds(CHUNK * f, CHUNK)
        for n in range(NCP):
            cs = pl.ds(COLP * n, COLP)
            part[rows, cs] = jnp.dot(hid[...], wd[:, cs], preferred_element_type=F32).astype(BF)
            for k in range(2):
                z_d2d(f, k, n).start()
            if n > 0:
                z_finish(f, n - 1)

    def output_rows(f):
        for n in range(NCP):
            z_x(f, n).wait_recv()
        keep_row = pl.multiple_of(QTR * chip, QTR)
        for j in range(QTR // ROWP):
            z = (ssum[f, pl.ds(keep_row + ROWP * j, ROWP), :].astype(F32) + rxz[f, pl.ds(ROWP * j, ROWP), :].astype(F32)).astype(BF).astype(F32)
            sl = pl.ds(QTR * f + ROWP * j, ROWP)
            out[0, sl, :] = (resid[chip, sl, :].astype(F32) + rms_rows(z, gain4).astype(F32)).astype(BF)

    embed_chunk(0)
    wg_cp.start()
    wu_cp.start()
    for cp in q_cps:
        cp.wait()
    qkv_chunk(0)
    attend_chunk(0)
    wo_cp.wait()
    out_chunk(0)
    wd_cp.start()
    embed_chunk(1)
    qkv_chunk(1)
    attend_chunk(1)
    out_chunk(1)
    mid_block(0, 0)
    mid_block(0, 1)
    wg_cp.wait()
    wu_cp.wait()
    wd_cp.wait()
    mid_block(1, 0)
    mid_arrive(0)
    up_part(0, 0, FFN // UPB)
    mid_block(1, 1)
    for k in range(2):
        for n in range(NCP):
            y_d2d(k, n).wait_send()
        for f in range(2):
            y_x(k, f).wait_send()
    down_part(0)
    mid_arrive(1)
    up_part(1, 0, 1)
    z_finish(0, NCP - 1)
    up_part(1, 1, FFN // UPB)
    down_part(1)
    z_finish(1, NCP - 1)
    output_rows(0)
    output_rows(1)
    for f in range(2):
        for k in range(2):
            for j in range(QTR // ROWP):
                m_d2d(k, f, j).wait_send()
            for n in range(NCP):
                z_d2d(f, k, n).wait_send()
        for n in range(NCP):
            z_x(f, n).wait_send()


def solution(mesh):
    in_specs = (P("dp", None), P("dp", None), P("tp", None), P(None, "tp", None), P(None, "tp", None), P(None, "tp", None), P("tp", None, None), P(None, "tp"), P(None, "tp"), P("tp", None), P(None), P(None), P(None), P(None))

    vm = pl.BlockSpec(memory_space=pltpu.VMEM)
    hb = pl.BlockSpec(memory_space=pl.ANY)
    dma = pltpu.SemaphoreType.DMA
    kernel = pl.pallas_call(
        layer_kernel,
        out_shape=jax.ShapeDtypeStruct((1, HALF, DIM), BF),
        in_specs=[hb, vm, vm, vm, vm] + [hb] * 7 + [vm] * 4,
        out_specs=vm,
        scratch_shapes=[
            pltpu.VMEM((DIM, 1280), BF),
            pltpu.VMEM((768, DIM), BF),
            pltpu.VMEM((DIM, FFN), BF),
            pltpu.VMEM((DIM, FFN), BF),
            pltpu.VMEM((FFN, DIM), BF),
            pltpu.VMEM((SEQ, DIM), BF),
            pltpu.VMEM((2, HALF, DIM), BF),
            pltpu.VMEM((2, HALF, DIM), BF),
            pltpu.VMEM((2, HALF, DIM), BF),
            pltpu.VMEM((2, HALF, DIM), BF),
            pltpu.VMEM((2, QTR, DIM), BF),
            pltpu.VMEM((SEQ, DIM), BF),
            pltpu.VMEM((2, HALF, DIM), BF),
            pltpu.VMEM((CHUNK, FFN), BF),
            pltpu.VMEM((6, CHUNK, 128), BF),
            pltpu.VMEM((2, SEQ, 128), BF),
            pltpu.VMEM((2, SEQ, 128), BF),
            pltpu.VMEM((CHUNK, 768), BF),
            pltpu.VMEM((512, 128), F32),
            pltpu.VMEM((SEQ, 1), F32),
            pltpu.VMEM((SEQ, 1), jnp.int32),
            dma((17,)),
            dma((2, NRP)), dma((2, NRP)),
            dma((2, NRP // 2)), dma((2, NRP // 2)),
            dma((2, NRP)), dma((2, NRP)),
            dma((2, NCP)), dma((2, NCP)),
            dma((2, 2)), dma((2, 2)),
            dma((2, 2, QTR // ROWP)), dma((2, 2, QTR // ROWP)),
            dma((2, 2, NCP)), dma((2, 2, NCP)),
            dma((2, NCP)), dma((2, NCP)),
        ],
        compiler_params=pltpu.CompilerParams(collective_id=0, has_side_effects=True, vmem_limit_bytes=67043328),
        name="decoder_layer",
    )

    def device_step(tokens, positions, embed_block, w_query, w_key, w_value, w_out, w_gate, w_up, w_down, g1, g2, g3, g4):
        dev_rank = lax.axis_index("tp")
        vocab_local, model_dim = embed_block.shape
        ids = tokens[0] - dev_rank * vocab_local
        in_block = (ids >= 0) & (ids < vocab_local)
        spread = jnp.arange(SEQ, dtype=jnp.int32) * (vocab_local // SEQ)
        looked = jnp.take(embed_block, jnp.where(in_block, ids, spread), axis=0, mode="clip")
        half = jnp.arange(128, dtype=jnp.int32) % 64
        inv_freq = ROPE_BASE ** (-2.0 * half.astype(F32) / 128)
        angles = positions[0].astype(F32)[:, None] * inv_freq
        cos_tab = jnp.cos(angles)
        sin_tab = jnp.sin(angles) * jnp.where(jnp.arange(128) < 64, -1.0, 1.0).astype(F32)
        return kernel(looked, tokens, positions, cos_tab, sin_tab,
                      w_query.transpose(1, 0, 2), w_key.reshape(2 * model_dim, 128), w_value.reshape(2 * model_dim, 128), w_out.reshape(768, model_dim),
                      w_gate, w_up, w_down, g1[None], g2[None], g3[None], g4[None])

    return jax.shard_map(device_step, mesh=mesh, in_specs=in_specs, out_specs=P("dp", "tp", None), check_vma=False)
```
